8 devices in a mesh: dp: 1 (over z), tp: 8 (over y, x, core).
Axes of the slice: x: 2, y: 2, z: 1, core: 2. Of those that a mesh axis runs over, the one named last changes fastest.
Arguments:
- x: bfloat16 [512, 2048], P('dp')
- k_cache: bfloat16 [512, 64, 16, 128], P('dp', None, 'tp')
- v_cache: bfloat16 [512, 64, 16, 128], P('dp', None, 'tp')
- positions: int32 [512], P('dp')
- att_ids: int32 [512, 2], P('dp')
- mlp_ids: int32 [512, 2], P('dp')
- norm_att: float32 [2048], replicated
- w_kv: bfloat16 [2048, 16, 256], P(None, 'tp')
- router_att: bfloat16 [2048, 8], replicated
- w_query: bfloat16 [8, 2048, 2048], P(None, None, 'tp')
- w_out: bfloat16 [8, 2048, 2048], P(None, 'tp')
- norm_mlp: float32 [2048], replicated
- router_mlp: bfloat16 [2048, 8], replicated
- w_gate: bfloat16 [8, 2048, 5632], P('tp')
- w_up: bfloat16 [8, 2048, 5632], P('tp')
- w_down: bfloat16 [8, 5632, 2048], P('tp')
Outputs:
- output 1: bfloat16 [512, 2048], P('dp')
- output 2: bfloat16 [512, 64, 16, 128], P('dp', None, 'tp')
- output 3: bfloat16 [512, 64, 16, 128], P('dp', None, 'tp')
All inputs are finite; a program needn't handle non-finite values.
Results may differ from the reference program's by a relative error of at most 0.012683.
Values are sent between devices in bfloat16 or wider.
A program may use at most 1 GiB of HBM per device.

```python
import jax
import jax.numpy as jnp
from jax import lax

HIDDEN = 2048
KV_HEADS = 16
HEAD_DIM = 128
ATT_EXPERTS = 8
MLP_EXPERTS = 8
FFN_WIDTH = 5632
TOKENS = 512
CACHE_LEN = 64

QUERY_WIDTH = KV_HEADS * HEAD_DIM
NORM_EPS = 1e-6
ROPE_BASE = 10000.0


def draw_pair(base_key, experts, skewed):
    key_first, key_offset, key_hot, key_share, key_coin = jax.random.split(base_key, 5)
    first_pick = jax.random.randint(key_first, (TOKENS,), 0, experts)
    if skewed:
        hot_id = jax.random.randint(key_hot, (), 0, experts)
        hot_share = jax.random.randint(key_share, (), 40, 61)
        coin_flip = jax.random.randint(key_coin, (TOKENS,), 0, 100)
        first_pick = jnp.where(coin_flip < hot_share, hot_id, first_pick)
    offset = jax.random.randint(key_offset, (TOKENS,), 1, experts)
    token_index = jnp.arange(TOKENS)
    forced = (token_index < experts) & (token_index != first_pick)
    second_pick = jnp.where(forced, token_index, (first_pick + offset) % experts)
    return jnp.stack([first_pick, second_pick], axis=1).astype(jnp.int32)


def draw_positions(base_key):
    positions = jax.random.randint(base_key, (TOKENS,), CACHE_LEN // 4, CACHE_LEN)
    return positions.at[0].set(CACHE_LEN - 1).at[1].set(CACHE_LEN // 4).astype(jnp.int32)


def setup_inputs(seed: int = 0, part: int = 0) -> dict:
    shared_keys = jax.random.split(jax.random.key(seed), 10)
    part_keys = jax.random.split(jax.random.fold_in(jax.random.key(seed + 1), part), 6)
    cache_shape = (TOKENS, CACHE_LEN, KV_HEADS, HEAD_DIM)
    x = jax.random.normal(part_keys[0], (TOKENS, HIDDEN), jnp.float32).astype(jnp.bfloat16)
    k_cache = jax.random.normal(part_keys[1], cache_shape, jnp.float32).astype(jnp.bfloat16)
    value_mean = jax.random.normal(part_keys[2], (TOKENS, 1, KV_HEADS, HEAD_DIM), jnp.float32)
    value_noise = jax.random.normal(part_keys[3], cache_shape, jnp.float32)
    v_cache = (0.8 * value_mean + 0.6 * value_noise).astype(jnp.bfloat16)
    positions = draw_positions(part_keys[4])
    choice_keys = jax.random.split(part_keys[5], 2)
    att_ids = draw_pair(choice_keys[0], ATT_EXPERTS, False)
    mlp_ids = draw_pair(choice_keys[1], MLP_EXPERTS, True)
    norm_att = 1.0 + 0.3 * jax.random.normal(shared_keys[0], (HIDDEN,), jnp.float32)
    w_kv = (jax.random.normal(shared_keys[1], (HIDDEN, KV_HEADS, 2 * HEAD_DIM), jnp.float32) * HIDDEN ** -0.5).astype(jnp.bfloat16)
    router_att = (jax.random.normal(shared_keys[2], (HIDDEN, ATT_EXPERTS), jnp.float32) * 0.5 * HIDDEN ** -0.5).astype(jnp.bfloat16)
    w_query = (jax.random.normal(shared_keys[3], (ATT_EXPERTS, HIDDEN, QUERY_WIDTH), jnp.float32) * HIDDEN ** -0.5).astype(jnp.bfloat16)
    w_out = (jax.random.normal(shared_keys[4], (ATT_EXPERTS, QUERY_WIDTH, HIDDEN), jnp.float32) * QUERY_WIDTH ** -0.5).astype(jnp.bfloat16)
    norm_mlp = 1.0 + 0.3 * jax.random.normal(shared_keys[5], (HIDDEN,), jnp.float32)
    router_mlp = (jax.random.normal(shared_keys[6], (HIDDEN, MLP_EXPERTS), jnp.float32) * 0.5 * HIDDEN ** -0.5).astype(jnp.bfloat16)
    w_gate = (jax.random.normal(shared_keys[7], (MLP_EXPERTS, HIDDEN, FFN_WIDTH), jnp.float32) * HIDDEN ** -0.5).astype(jnp.bfloat16)
    w_up = (jax.random.normal(shared_keys[8], (MLP_EXPERTS, HIDDEN, FFN_WIDTH), jnp.float32) * HIDDEN ** -0.5).astype(jnp.bfloat16)
    w_down = (jax.random.normal(shared_keys[9], (MLP_EXPERTS, FFN_WIDTH, HIDDEN), jnp.float32) * FFN_WIDTH ** -0.5).astype(jnp.bfloat16)
    return {'x': x, 'k_cache': k_cache, 'v_cache': v_cache, 'positions': positions, 'att_ids': att_ids, 'mlp_ids': mlp_ids, 'norm_att': norm_att, 'w_kv': w_kv, 'router_att': router_att, 'w_query': w_query, 'w_out': w_out, 'norm_mlp': norm_mlp, 'router_mlp': router_mlp, 'w_gate': w_gate, 'w_up': w_up, 'w_down': w_down}


def rms_norm(x, gain):
    values = x.astype(jnp.float32)
    inv_rms = lax.rsqrt(jnp.mean(values * values, axis=-1, keepdims=True) + NORM_EPS)
    return (values * inv_rms * gain).astype(jnp.bfloat16)


def rope_tables(positions):
    half_dim = HEAD_DIM // 2
    inv_freq = ROPE_BASE ** (-(jnp.arange(half_dim, dtype=jnp.float32) * 2.0 / HEAD_DIM))
    angles = positions.astype(jnp.float32)[:, None] * inv_freq[None, :]
    return jnp.cos(angles), jnp.sin(angles)


def apply_rope(vectors, cos_table, sin_table):
    half_dim = vectors.shape[-1] // 2
    first_half = vectors[..., :half_dim]
    second_half = vectors[..., half_dim:]
    return jnp.concatenate([first_half * cos_table - second_half * sin_table, second_half * cos_table + first_half * sin_table], axis=-1)


def reference(x, k_cache, v_cache, positions, att_ids, mlp_ids, norm_att, w_kv, router_att, w_query, w_out, norm_mlp, router_mlp, w_gate, w_up, w_down):
    hidden = rms_norm(x, norm_att)
    kv_new = jnp.dot(hidden, w_kv.reshape(HIDDEN, KV_HEADS * 2 * HEAD_DIM), preferred_element_type=jnp.float32).reshape(TOKENS, KV_HEADS, 2 * HEAD_DIM)
    cos_table, sin_table = rope_tables(positions)
    key_new = apply_rope(kv_new[:, :, :HEAD_DIM], cos_table[:, None, :], sin_table[:, None, :]).astype(jnp.bfloat16)
    value_new = kv_new[:, :, HEAD_DIM:].astype(jnp.bfloat16)
    slot_index = jnp.arange(CACHE_LEN)
    at_slot = (slot_index[None, :] == positions[:, None])[:, :, None, None]
    keys_all = jnp.where(at_slot, key_new[:, None, :, :], k_cache)
    values_all = jnp.where(at_slot, value_new[:, None, :, :], v_cache)
    att_logits = jnp.dot(hidden, router_att, preferred_element_type=jnp.float32)
    att_gates = jax.nn.softmax(jnp.take_along_axis(att_logits, att_ids, axis=1), axis=-1)
    query_all = jnp.einsum('bd,edc->bec', hidden.astype(jnp.float32), w_query.astype(jnp.float32))
    query_sel = jnp.take_along_axis(query_all, att_ids[:, :, None], axis=1).reshape(TOKENS, 2, KV_HEADS, HEAD_DIM)
    query_rot = apply_rope(query_sel, cos_table[:, None, None, :], sin_table[:, None, None, :]).astype(jnp.bfloat16)
    scores = jnp.einsum('bknd,bsnd->bkns', query_rot.astype(jnp.float32), keys_all.astype(jnp.float32)) * HEAD_DIM ** -0.5
    visible = (slot_index[None, :] <= positions[:, None])[:, None, None, :]
    weights = jax.nn.softmax(jnp.where(visible, scores, -1e30), axis=-1).astype(jnp.bfloat16)
    attended = jnp.einsum('bkns,bsnd->bknd', weights.astype(jnp.float32), values_all.astype(jnp.float32)).astype(jnp.bfloat16).reshape(TOKENS, 2, QUERY_WIDTH)
    att_onehot = (att_ids[:, :, None] == jnp.arange(ATT_EXPERTS)[None, None, :]).astype(jnp.float32)
    out_slots = jnp.einsum('bke,bkc->bec', att_onehot, attended.astype(jnp.float32))
    projected = jnp.einsum('bec,ecd->bed', out_slots, w_out.astype(jnp.float32))
    att_dense = jnp.einsum('bke,bk->be', att_onehot, att_gates)
    att_sum = jnp.einsum('be,bed->bd', att_dense, projected)
    x_mid = (x.astype(jnp.float32) + att_sum).astype(jnp.bfloat16)
    normed = rms_norm(x_mid, norm_mlp)
    mlp_logits = jnp.dot(normed, router_mlp, preferred_element_type=jnp.float32)
    mlp_gates = jax.nn.softmax(jnp.take_along_axis(mlp_logits, mlp_ids, axis=1), axis=-1)
    mlp_onehot = (mlp_ids[:, :, None] == jnp.arange(MLP_EXPERTS)[None, None, :]).astype(jnp.float32)
    mlp_dense = jnp.einsum('bke,bk->be', mlp_onehot, mlp_gates)

    def expert_step(running_sum, expert_inputs):
        gate_mat, up_mat, down_mat, weight_col = expert_inputs
        gate_val = jnp.dot(normed, gate_mat, preferred_element_type=jnp.float32)
        up_val = jnp.dot(normed, up_mat, preferred_element_type=jnp.float32)
        activation = (jax.nn.silu(gate_val) * up_val).astype(jnp.bfloat16)
        down_out = jnp.dot(activation, down_mat, preferred_element_type=jnp.float32)
        return running_sum + weight_col[:, None] * down_out, None

    mlp_sum, _ = lax.scan(expert_step, jnp.zeros((TOKENS, HIDDEN), jnp.float32), (w_gate, w_up, w_down, mlp_dense.T))
    x_out = (x_mid.astype(jnp.float32) + mlp_sum).astype(jnp.bfloat16)
    return x_out, keys_all, values_all
```

```python
import functools

import jax
import jax.numpy as jnp
from jax import lax
from jax.experimental import pallas as pl
from jax.experimental.pallas import tpu as pltpu
from jax.sharding import PartitionSpec as P

NORM_EPS = 1e-6
ROPE_BASE = 10000.0
NEG = -1e30
VMEM_LIMIT = 60 * 1024 * 1024
ROW_SIZES = (256, 320, 384, 512)


def rms_rows(x, gain):
    values = x.astype(jnp.float32)
    inv_rms = lax.rsqrt(jnp.mean(values * values, axis=-1, keepdims=True) + NORM_EPS)
    return (values * inv_rms * gain).astype(jnp.bfloat16)


def project_kernel(x_ref, gain_ref, router_ref, ids_ref, cos_ref, sin_ref, wkv_ref, wq_ref, q_ref, k_ref, v_ref, gate_ref, h_ref, acc_ref):
    step = pl.program_id(0)
    experts = pl.num_programs(0)
    tokens = x_ref.shape[0]
    dim = cos_ref.shape[1]
    heads = k_ref.shape[0] // tokens

    def rope(vec):
        return vec * cos_ref[...] + pltpu.roll(vec, dim // 2, 1) * sin_ref[...]

    @pl.when(step == 0)
    def _():
        h_ref[...] = rms_rows(x_ref[...], gain_ref[...])
        acc_ref[...] = jnp.zeros_like(acc_ref)
        for n in range(heads):
            kv = jnp.dot(h_ref[...], wkv_ref[n], preferred_element_type=jnp.float32)
            k_ref[pl.ds(n, tokens, stride=heads), :] = rope(kv[:, :dim])
            v_ref[pl.ds(n, tokens, stride=heads), :] = kv[:, dim:]
        logits = lax.dot_general(h_ref[...], router_ref[...], (((1,), (1,)), ((), ())), preferred_element_type=jnp.float32)
        lane = lax.broadcasted_iota(jnp.int32, logits.shape, 1)
        is_first = lane == ids_ref[:, 0:1]
        is_second = lane == ids_ref[:, 1:2]
        first = jnp.sum(jnp.where(is_first, logits, 0.0), axis=1, keepdims=True)
        second = jnp.sum(jnp.where(is_second, logits, 0.0), axis=1, keepdims=True)
        top = jnp.maximum(first, second)
        e_first = jnp.exp(first - top)
        e_second = jnp.exp(second - top)
        total = e_first + e_second
        gate_ref[...] = jnp.where(is_first, e_first / total, 0.0) + jnp.where(is_second, e_second / total, 0.0)

    query = jnp.dot(h_ref[...], wq_ref[0], preferred_element_type=jnp.float32)
    for k in range(2):
        acc_ref[k] = jnp.where(ids_ref[:, k:k + 1] == step, query, acc_ref[k])

    @pl.when(step == experts - 1)
    def _():
        for k in range(2):
            for n in range(heads):
                q_ref[pl.ds(k * heads + n, tokens, stride=2 * heads), :] = rope(acc_ref[k, :, n * dim:(n + 1) * dim])


def project(x, gain, router_t, ids, cos, sin, w_kv, w_query):
    tokens, width = x.shape
    experts = w_query.shape[0]
    heads, dim = w_kv.shape[0], w_kv.shape[2] // 2
    full = lambda *shape: pl.BlockSpec(shape, lambda i: (0,) * len(shape))
    return pl.pallas_call(
        project_kernel,
        grid=(experts,),
        in_specs=[full(tokens, width), full(1, width), full(experts, width), full(tokens, 2), full(tokens, dim), full(tokens, dim),
                  full(heads, width, 2 * dim), pl.BlockSpec((1, width, heads * dim), lambda i: (i, 0, 0))],
        out_specs=[full(2 * heads * tokens, dim), full(heads * tokens, dim), full(heads * tokens, dim), full(tokens, experts)],
        out_shape=[jax.ShapeDtypeStruct((2 * heads * tokens, dim), jnp.float32), jax.ShapeDtypeStruct((heads * tokens, dim), jnp.float32),
                   jax.ShapeDtypeStruct((heads * tokens, dim), jnp.float32), jax.ShapeDtypeStruct((tokens, experts), jnp.float32)],
        scratch_shapes=[pltpu.VMEM((tokens, width), jnp.bfloat16), pltpu.VMEM((2, tokens, heads * dim), jnp.float32)],
        compiler_params=pltpu.CompilerParams(vmem_limit_bytes=VMEM_LIMIT),
        name='project',
    )(x, gain, router_t, ids, cos, sin, w_kv, w_query)


BLOCK = 32
SLOTS = 4
AHEAD = 2
GROUP = 2


def attend_kernel(pos_ref, q_ref, kn_ref, vn_ref, k_hbm, v_hbm, o_ref, ko_hbm, vo_hbm, kbuf, vbuf, in_sem, out_sem):
    tokens, rows, dim = k_hbm.shape
    blocks = tokens // BLOCK
    heads = kn_ref.shape[0] // tokens
    per_token = q_ref.shape[0] // tokens
    scale = dim ** -0.5

    def load(i, slot):
        span = pl.ds(i * BLOCK, BLOCK)
        return (pltpu.make_async_copy(k_hbm.at[span], kbuf.at[slot], in_sem.at[slot, 0]),
                pltpu.make_async_copy(v_hbm.at[span], vbuf.at[slot], in_sem.at[slot, 1]))

    def store(i, slot):
        span = pl.ds(i * BLOCK, BLOCK)
        return (pltpu.make_async_copy(kbuf.at[slot], ko_hbm.at[span], out_sem.at[slot, 0]),
                pltpu.make_async_copy(vbuf.at[slot], vo_hbm.at[span], out_sem.at[slot, 1]))

    for i in range(AHEAD):
        for copy in load(i, i):
            copy.start()

    tile_row = lax.broadcasted_iota(jnp.int32, (16, dim), 0)
    lanes = GROUP * rows
    q_rows = GROUP * per_token
    lane = lax.broadcasted_iota(jnp.int32, (q_rows, lanes), 1)
    row = lax.broadcasted_iota(jnp.int32, (q_rows, lanes), 0)
    match = (lane // rows == row // per_token) & (lane % heads == row % heads)
    slot_of = jnp.where(match, (lane % rows) // heads, rows)
    row_token = row // per_token

    def body(i, carry):
        slot = lax.rem(i, SLOTS)
        later = i + AHEAD

        @pl.when(later < blocks)
        def _():
            later_slot = lax.rem(later, SLOTS)

            @pl.when(later >= SLOTS)
            def _():
                for copy in store(later - SLOTS, later_slot):
                    copy.wait()
            for copy in load(later, later_slot):
                copy.start()

        for copy in load(i, slot):
            copy.wait()
        kb = kbuf.at[slot]
        vb = vbuf.at[slot]
        base_token = i * BLOCK
        positions = [pos_ref[base_token + t] for t in range(BLOCK)]
        for t in range(BLOCK):
            p = positions[t]
            start = pl.multiple_of((p // 8) * 16, 16)
            local = (p % 8) * heads
            for buf, new in ((kb, kn_ref), (vb, vn_ref)):
                tile = buf[t, pl.ds(start, 16), :].astype(jnp.float32)
                for n in range(heads):
                    tile = jnp.where(tile_row == local + n, new[pl.ds(heads * (base_token + t) + n, 1), :], tile)
                buf[t, pl.ds(start, 16), :] = tile.astype(jnp.bfloat16)
        for g in range(BLOCK // GROUP):
            first = (base_token + g * GROUP) * per_token
            q = q_ref[pl.ds(pl.multiple_of(first, q_rows), q_rows), :].astype(jnp.bfloat16)
            keys = kb[g * GROUP:(g + 1) * GROUP].reshape(lanes, dim)
            scores = lax.dot_general(q, keys, (((1,), (1,)), ((), ())), preferred_element_type=jnp.float32) * scale
            limit = positions[g * GROUP]
            for t in range(1, GROUP):
                limit = jnp.where(row_token == t, positions[g * GROUP + t], limit)
            scores = jnp.where(slot_of <= limit, scores, NEG)
            weights = jnp.exp(scores - jnp.max(scores, axis=1, keepdims=True))
            weights = (weights / jnp.sum(weights, axis=1, keepdims=True)).astype(jnp.bfloat16)
            values = vb[g * GROUP:(g + 1) * GROUP].reshape(lanes, dim)
            o_ref[pl.ds(pl.multiple_of(first, q_rows), q_rows), :] = jnp.dot(weights, values, preferred_element_type=jnp.float32)
        for copy in store(i, slot):
            copy.start()
        return carry

    lax.fori_loop(0, blocks, body, 0)
    for i in range(blocks - SLOTS, blocks):
        for copy in store(i, i % SLOTS):
            copy.wait()


def attend(positions, q, k_new, v_new, k_cache, v_cache):
    tokens, rows, dim = k_cache.shape
    vmem = pl.BlockSpec(memory_space=pltpu.VMEM)
    hbm = pl.BlockSpec(memory_space=pl.ANY)
    return pl.pallas_call(
        attend_kernel,
        in_specs=[pl.BlockSpec(memory_space=pltpu.SMEM), vmem, vmem, vmem, hbm, hbm],
        out_specs=[vmem, hbm, hbm],
        out_shape=[jax.ShapeDtypeStruct(q.shape, jnp.float32), jax.ShapeDtypeStruct(k_cache.shape, k_cache.dtype), jax.ShapeDtypeStruct(v_cache.shape, v_cache.dtype)],
        scratch_shapes=[pltpu.VMEM((SLOTS, BLOCK, rows, dim), jnp.bfloat16), pltpu.VMEM((SLOTS, BLOCK, rows, dim), jnp.bfloat16),
                        pltpu.SemaphoreType.DMA((SLOTS, 2)), pltpu.SemaphoreType.DMA((SLOTS, 2))],
        compiler_params=pltpu.CompilerParams(vmem_limit_bytes=VMEM_LIMIT),
        name='attend',
    )(positions, q, k_new, v_new, k_cache, v_cache)


def combine_kernel(o_ref, ids_ref, gate_ref, w_ref, out_ref, acc_ref):
    step = pl.program_id(0)
    experts = pl.num_programs(0)
    tokens = ids_ref.shape[0]
    per_token = o_ref.shape[0] // tokens
    heads = per_token // 2
    parts = []
    for n in range(heads):
        first = o_ref[pl.ds(n, tokens, stride=per_token), :]
        second = o_ref[pl.ds(heads + n, tokens, stride=per_token), :]
        parts.append(jnp.where(ids_ref[:, 0:1] == step, first, jnp.where(ids_ref[:, 1:2] == step, second, 0.0)).astype(jnp.bfloat16))
    rows = jnp.concatenate(parts, axis=1)
    projected = jnp.dot(rows, w_ref[0], preferred_element_type=jnp.float32)
    lane = lax.broadcasted_iota(jnp.int32, gate_ref.shape, 1)
    gate = jnp.sum(jnp.where(lane == step, gate_ref[...], 0.0), axis=1, keepdims=True)

    @pl.when(step == 0)
    def _():
        acc_ref[...] = gate * projected

    @pl.when((step > 0) & (step < experts - 1))
    def _():
        acc_ref[...] += gate * projected

    @pl.when(step == experts - 1)
    def _():
        out_ref[...] = (acc_ref[...] + gate * projected).astype(jnp.bfloat16)


def combine(o, ids, gates, w_out):
    experts, depth, width = w_out.shape
    tokens = ids.shape[0]
    full = lambda *shape: pl.BlockSpec(shape, lambda i: (0,) * len(shape))
    return pl.pallas_call(
        combine_kernel,
        grid=(experts,),
        in_specs=[full(*o.shape), full(tokens, 2), full(tokens, experts), pl.BlockSpec((1, depth, width), lambda i: (i, 0, 0))],
        out_specs=full(tokens, width),
        out_shape=jax.ShapeDtypeStruct((tokens, width), jnp.bfloat16),
        scratch_shapes=[pltpu.VMEM((tokens, width), jnp.float32)],
        compiler_params=pltpu.CompilerParams(vmem_limit_bytes=VMEM_LIMIT),
        name='combine',
    )(o, ids, gates, w_out)


def reduce_kernel(part_ref, base_ref, out_ref, pair_buf, send_buf, chip_buf, pair_send, pair_recv, chip_send, chip_recv, own_send, own_recv, fwd_send, fwd_recv):
    me = lax.axis_index('tp')
    rows = part_ref.shape[0] // 8
    core = me % 2
    x = (me // 2) % 2
    y = me // 4
    partner = me + 1 - 2 * core

    def chip(k):
        return 2 * ((y + k // 2) % 2) + (x + k % 2) % 2

    def span(device):
        return pl.ds(pl.multiple_of(device * rows, rows), rows)

    barrier = pltpu.get_barrier_semaphore()
    for device in [partner] + [2 * chip(k) + core for k in (1, 2, 3)]:
        pl.semaphore_signal(barrier, inc=1, device_id={'tp': device}, device_id_type=pl.DeviceIdType.MESH)
    pl.semaphore_wait(barrier, 4)

    def remote(src, dst, send, recv, device):
        return pltpu.make_async_remote_copy(src_ref=src, dst_ref=dst, send_sem=send, recv_sem=recv, device_id={'tp': device}, device_id_type=pl.DeviceIdType.MESH)

    order = (3, 1, 2, 0)
    pair = {}
    for k in order:
        pair[k] = remote(part_ref.at[span(2 * chip(k) + 1 - core)], pair_buf.at[k], pair_send.at[k], pair_recv.at[k], partner)
        pair[k].start()
    across = {}
    for k in order[:3]:
        pair[k].wait_recv()
        send_buf[k - 1] = (part_ref[span(2 * chip(k) + core), :].astype(jnp.float32) + pair_buf[k].astype(jnp.float32)).astype(jnp.bfloat16)
        across[k] = remote(send_buf.at[k - 1], chip_buf.at[k - 1], chip_send.at[k - 1], chip_recv.at[k - 1], 2 * chip(k) + core)
        across[k].start()
    pair[0].wait_recv()
    total = part_ref[span(me), :].astype(jnp.float32) + pair_buf[0].astype(jnp.float32)
    for k in (1, 2, 3):
        across[k].wait_recv()
        total = total + chip_buf[k - 1].astype(jnp.float32)
    out_ref[span(me), :] = (base_ref[span(me), :].astype(jnp.float32) + total).astype(jnp.bfloat16)

    own = {}
    for k in order[:3]:
        own[k] = remote(out_ref.at[span(me)], out_ref.at[span(me)], own_send.at[k], own_recv.at[k], 2 * chip(k) + core)
        own[k].start()
    forward = {0: remote(out_ref.at[span(me)], out_ref.at[span(me)], fwd_send.at[0], fwd_recv.at[0], partner)}
    forward[0].start()
    for k in (1, 2, 3):
        block = span(2 * chip(k) + core)
        own[k].wait_recv()
        forward[k] = remote(out_ref.at[block], out_ref.at[block], fwd_send.at[k], fwd_recv.at[k], partner)
        forward[k].start()
    for k in range(4):
        forward[k].wait_recv()
    for k in range(4):
        forward[k].wait_send()
        pair[k].wait_send()
    for k in (1, 2, 3):
        own[k].wait_send()
        across[k].wait_send()


def reduce_add(part, base, collective_id):
    tokens, width = part.shape
    rows = tokens // 8
    vmem = pl.BlockSpec(memory_space=pltpu.VMEM)
    return pl.pallas_call(
        reduce_kernel,
        in_specs=[vmem, vmem],
        out_specs=vmem,
        out_shape=jax.ShapeDtypeStruct((tokens, width), jnp.bfloat16),
        scratch_shapes=[pltpu.VMEM((4, rows, width), jnp.bfloat16), pltpu.VMEM((3, rows, width), jnp.bfloat16), pltpu.VMEM((3, rows, width), jnp.bfloat16)]
        + [pltpu.SemaphoreType.DMA((n,)) for n in (4, 4, 3, 3, 4, 4, 4, 4)],
        compiler_params=pltpu.CompilerParams(collective_id=collective_id, has_side_effects=True, vmem_limit_bytes=VMEM_LIMIT),
        name=f'reduce_{collective_id}',
    )(part, base)


def expert_kernel(first_ref, x_ref, gain_ref, router_ref, ids_ref, wg_ref, wu_ref, wd_ref, out_ref, rank_ref, gate_ref, rows_ref, acc_ref, count_ref):
    step = pl.program_id(0)
    steps = pl.num_programs(0)
    tokens, width = x_ref.shape
    experts = router_ref.shape[0]
    mine = first_ref[0]

    @pl.when(step == 0)
    def _():
        normed = rms_rows(x_ref[...], gain_ref[...])
        logits = lax.dot_general(router_ref[...], normed, (((1,), (1,)), ((), ())), preferred_element_type=jnp.float32)
        id_first = ids_ref[0:1, :]
        id_second = ids_ref[1:2, :]
        index = lax.broadcasted_iota(jnp.int32, (experts, tokens), 0)
        first = jnp.sum(jnp.where(index == id_first, logits, 0.0), axis=0, keepdims=True)
        second = jnp.sum(jnp.where(index == id_second, logits, 0.0), axis=0, keepdims=True)
        top = jnp.maximum(first, second)
        e_first = jnp.exp(first - top)
        e_second = jnp.exp(second - top)
        total = e_first + e_second
        gate = jnp.where(id_first == mine, e_first / total, 0.0) + jnp.where(id_second == mine, e_second / total, 0.0)
        chosen = (id_first == mine) | (id_second == mine)
        flags = jnp.where(chosen, 1.0, 0.0)
        below = (lax.broadcasted_iota(jnp.int32, (tokens, tokens), 0) <= lax.broadcasted_iota(jnp.int32, (tokens, tokens), 1)).astype(jnp.bfloat16)
        counts = jnp.dot(jnp.broadcast_to(flags, (8, tokens)).astype(jnp.bfloat16), below, preferred_element_type=jnp.float32)[0:1, :]
        rank = jnp.where(chosen, counts.astype(jnp.int32) - 1, -1)
        rank_ref[...] = rank
        count_ref[0] = jnp.sum(chosen.astype(jnp.int32))
        pick = lax.broadcasted_iota(jnp.int32, (tokens, tokens), 0) == rank
        gate_ref[...] = jnp.sum(jnp.where(pick, gate, 0.0), axis=1, keepdims=True)
        rows_ref[...] = jnp.dot(pick.astype(jnp.bfloat16), normed, preferred_element_type=jnp.float32).astype(jnp.bfloat16)

    def run(size):
        rows = rows_ref[:size, :]
        gate_val = jnp.dot(rows, wg_ref[0], preferred_element_type=jnp.float32)
        up_val = jnp.dot(rows, wu_ref[0], preferred_element_type=jnp.float32)
        act = (jax.nn.silu(gate_val) * up_val).astype(jnp.bfloat16)
        down = jnp.dot(act, wd_ref[0], preferred_element_type=jnp.float32)

        @pl.when(step == 0)
        def _():
            acc_ref[:size, :] = down

        @pl.when(step > 0)
        def _():
            acc_ref[:size, :] += down

        @pl.when(step == steps - 1)
        def _():
            mixed = (acc_ref[:size, :] * gate_ref[:size, :]).astype(jnp.bfloat16)
            pick = (lax.broadcasted_iota(jnp.int32, (size, tokens), 0) == rank_ref[...]).astype(jnp.bfloat16)
            out_ref[...] = lax.dot_general(pick, mixed, (((0,), (0,)), ((), ())), preferred_element_type=jnp.float32).astype(jnp.bfloat16)

    count = count_ref[0]
    lower = -1
    for size in ROW_SIZES:
        upper = size if size < tokens else tokens
        pl.when((count > lower) & (count <= upper))(functools.partial(run, size))
        lower = upper


def expert(first, x, gain, router_t, ids_t, w_gate, w_up, w_down):
    tokens, width = x.shape
    ffn = w_gate.shape[2]
    tile = 512
    full = lambda *shape: pl.BlockSpec(shape, lambda i: (0,) * len(shape))
    return pl.pallas_call(
        expert_kernel,
        grid=(ffn // tile,),
        in_specs=[pl.BlockSpec(memory_space=pltpu.SMEM), full(tokens, width), full(1, width), full(*router_t.shape), full(2, tokens),
                  pl.BlockSpec((1, width, tile), lambda i: (0, 0, i)), pl.BlockSpec((1, width, tile), lambda i: (0, 0, i)),
                  pl.BlockSpec((1, tile, width), lambda i: (0, i, 0))],
        out_specs=full(tokens, width),
        out_shape=jax.ShapeDtypeStruct((tokens, width), jnp.bfloat16),
        scratch_shapes=[pltpu.VMEM((1, tokens), jnp.int32), pltpu.VMEM((tokens, 1), jnp.float32), pltpu.VMEM((tokens, width), jnp.bfloat16),
                        pltpu.VMEM((tokens, width), jnp.float32), pltpu.SMEM((1,), jnp.int32)],
        compiler_params=pltpu.CompilerParams(vmem_limit_bytes=VMEM_LIMIT),
        name='expert',
    )(first, x, gain, router_t, ids_t, w_gate, w_up, w_down)


def solution(mesh):
    def local_step(x, k_cache, v_cache, positions, att_ids, mlp_ids, norm_att, w_kv, router_att, w_query, w_out, norm_mlp, router_mlp, w_gate, w_up, w_down):
        tokens, slots, heads, dim = k_cache.shape
        half = dim // 2
        inv_freq = ROPE_BASE ** (-(jnp.arange(half, dtype=jnp.float32) * 2.0 / dim))
        angles = positions.astype(jnp.float32)[:, None] * inv_freq[None, :]
        cos, sin = jnp.cos(angles), jnp.sin(angles)
        cos = jnp.concatenate([cos, cos], axis=1)
        sin = jnp.concatenate([-sin, sin], axis=1)
        q, k_new, v_new, gates = project(x, norm_att[None, :], router_att.T, att_ids, cos, sin, w_kv.transpose(1, 0, 2), w_query)
        merged = (tokens, slots * heads, dim)
        attended, keys_all, values_all = attend(positions, q, k_new, v_new, k_cache.reshape(merged), v_cache.reshape(merged))
        part = combine(attended, att_ids, gates, w_out)
        x_mid = reduce_add(part, x, 0)
        first = lax.axis_index('tp').reshape(1)
        mlp_part = expert(first, x_mid, norm_mlp[None, :], router_mlp.T, mlp_ids.T, w_gate, w_up, w_down)
        x_out = reduce_add(mlp_part, x_mid, 1)
        return x_out, keys_all.reshape(k_cache.shape), values_all.reshape(v_cache.shape)

    token_spec = P('dp', None)
    cache_spec = P('dp', None, 'tp', None)
    expert_spec = P('tp', None, None)
    in_specs = (token_spec, cache_spec, cache_spec, P('dp'), token_spec, token_spec, P(), P(None, 'tp', None), P(), P(None, None, 'tp'), P(None, 'tp', None), P(), P(), expert_spec, expert_spec, expert_spec)
    out_specs = (token_spec, cache_spec, cache_spec)
    return jax.shard_map(local_step, mesh=mesh, in_specs=in_specs, out_specs=out_specs, check_vma=False)
```
